32 devices in a mesh: fsdp: 8 (over y, x, core), seq: 4 (over z).
Axes of the slice: x: 2, y: 2, z: 4, core: 2. Of those that a mesh axis runs over, the one named last changes fastest.
Arguments:
- tokens: bfloat16 [8192, 768], P(('fsdp', 'seq')), may hold values from -6 to 6
- segments: int32 [8, 1024], P('fsdp'), may hold values from 0 to 3, never falling along the last dimension, each value on 1 to 512 neighbouring positions
- cotangent: bfloat16 [8192, 768], P(('fsdp', 'seq')), may hold values from -6 to 6
- query_weight: float32 [768, 768], P(('fsdp', 'seq')), may hold values from -0.21875 to 0.21875
- query_bias: float32 [768], P(('fsdp', 'seq')), may hold values from -3 to 3
- key_weight: float32 [768, 768], P(('fsdp', 'seq')), may hold values from -0.21875 to 0.21875
- value_weight: float32 [768, 768], P(('fsdp', 'seq')), may hold values from -0.21875 to 0.21875
- value_bias: float32 [768], P(('fsdp', 'seq')), may hold values from -3 to 3
- mixer_weight: float32 [768, 768], P(('fsdp', 'seq')), may hold values from -1.5 to 1.5
- mixer_bias: float32 [768], P(('fsdp', 'seq')), may hold values from -1.75 to 1.75
- first_gain: float32 [768], P(('fsdp', 'seq')), may hold values from 0.5 to 1.5
- first_shift: float32 [768], P(('fsdp', 'seq')), may hold values from -1.75 to 1.75
- inner_weight: float32 [768, 3072], P(('fsdp', 'seq')), may hold values from -0.21875 to 0.21875
- inner_bias: float32 [3072], P(('fsdp', 'seq')), may hold values from -3 to 3
- outer_weight: float32 [3072, 768], P(('fsdp', 'seq')), may hold values from -0.15625 to 0.15625
- outer_bias: float32 [768], P(('fsdp', 'seq')), may hold values from -1.75 to 1.75
- second_gain: float32 [768], P(('fsdp', 'seq')), may hold values from 0.5 to 1.5
- second_shift: float32 [768], P(('fsdp', 'seq')), may hold values from -1.75 to 1.75
Outputs:
- layer_out: bfloat16 [8192, 768], P(('fsdp', 'seq'))
- tokens_grad: bfloat16 [8192, 768], P(('fsdp', 'seq'))
- query_weight_grad: float32 [768, 768], P(('fsdp', 'seq'))
- query_bias_grad: float32 [768], P(('fsdp', 'seq'))
- key_weight_grad: float32 [768, 768], P(('fsdp', 'seq'))
- value_weight_grad: float32 [768, 768], P(('fsdp', 'seq'))
- value_bias_grad: float32 [768], P(('fsdp', 'seq'))
- mixer_weight_grad: float32 [768, 768], P(('fsdp', 'seq'))
- mixer_bias_grad: float32 [768], P(('fsdp', 'seq'))
- first_gain_grad: float32 [768], P(('fsdp', 'seq'))
- first_shift_grad: float32 [768], P(('fsdp', 'seq'))
- inner_weight_grad: float32 [768, 3072], P(('fsdp', 'seq'))
- inner_bias_grad: float32 [3072], P(('fsdp', 'seq'))
- outer_weight_grad: float32 [3072, 768], P(('fsdp', 'seq'))
- outer_bias_grad: float32 [768], P(('fsdp', 'seq'))
- second_gain_grad: float32 [768], P(('fsdp', 'seq'))
- second_shift_grad: float32 [768], P(('fsdp', 'seq'))
The draws below stay inside these ranges and needn't reach their ends.
Inputs may be any that keep to these rules, and one draw needn't show every extreme that they name: `segments`: within each sequence the document numbers never fall; each document covers 1 to 512 positions, one of them exactly that many.
All inputs are finite; a program needn't handle non-finite values.
Results may differ from the reference program's by a relative error of at most 0.015.
The reference program's roundings to bfloat16 on the way count: a program that leaves them out, or rounds other values in their place, can miss the bound.
Values may be sent and summed in bfloat16 or wider, within the bound.
No kernel may reach another device: no remote copies, remote signals or barrier semaphores. Data moves between devices by JAX's collectives and lax.ppermute only.
A program may use at most 192 MiB of HBM per device.

```python
import math
import jax
import jax.numpy as jnp
import numpy as np
from jax import lax

D = 768
HEADS = 12
HD = 64
FF = 3072
SEQ_LEN = 1024
SEQS = 8
TOKENS = 8192


def spiked(values, key, source, target, parts, factor):
    def block_of(position):
        return (jnp.arange(values.shape[position]) // (values.shape[position] // parts)).reshape((-1,) + (1,) * (values.ndim - 1 - position))

    first = jax.random.permutation(key, parts)[block_of(target)]
    other_side = (block_of(target) + parts // 2) % parts
    return jnp.where((block_of(source) == first) | (block_of(source) == other_side), factor * values, values)


def block_scale(own_key, dims, shards, least, largest):
    def one(axis_at, blocks):
        heights = jax.random.uniform(jax.random.fold_in(jax.random.fold_in(own_key, 6), axis_at), (blocks,), jnp.float32, least / len(shards), largest / len(shards))
        return jnp.repeat(jnp.exp(heights), dims[axis_at] // blocks).reshape((-1,) + (1,) * (len(dims) - axis_at - 1))

    loudness = one(*shards[0])
    for cut in shards[1:]:
        loudness = loudness * one(*cut)
    return loudness


def length_profile(count, total, bound, slope):
    loads = [(1 << 20) // math.isqrt(grade ** slope) + 1 for grade in range(2, count + 1)]
    spare, holding = total - bound - (count - 1), [1] * (count - 1)
    while spare > 0:
        candidates = [i for i in range(count - 1) if holding[i] < bound]
        mass, left = sum([loads[i] for i in candidates]), spare
        for i in candidates:
            extra = min(bound - holding[i], max(1, left * loads[i] // mass), spare)
            holding[i] = holding[i] + extra
            spare = spare - extra
    return np.array([bound] + holding)


def uneven(own_key, count, total, bound, lean):
    if count == 2:
        one = jax.random.randint(own_key, (), max(1, total - bound), min(bound, total - 1) + 1)
        return jnp.stack([one, total - one])
    lengths = jnp.asarray(length_profile(count, total, bound, lean), jnp.int32)
    twos = (count - 1) // 2
    giver, receiver = lengths[1:1 + 2 * twos:2], lengths[2:2 + 2 * twos:2]
    slack = jnp.minimum(giver - 1, bound - receiver)
    moved = jax.random.randint(jax.random.fold_in(own_key, 1), (twos,), 0, 1 << 20) % (slack + 1)
    lengths = lengths.at[1:1 + 2 * twos:2].set(giver - moved).at[2:2 + 2 * twos:2].set(receiver + moved)
    return lengths[jax.random.permutation(jax.random.fold_in(own_key, 2), count)]


def gaussian(key, shape, deviation, reach, split=(), kind=jnp.bfloat16):
    factor_of = block_scale(key, shape, split, -0.22, 0.18) if split else 1.0
    array = jax.random.normal(key, shape, jnp.float32) * deviation * factor_of
    return jnp.minimum(jnp.maximum(array, -reach), reach).astype(kind)


def noise_with(key, dims, deviation, reach, pieces, heavy, dtype=jnp.bfloat16):
    drawn = deviation * jax.random.normal(key, dims, jnp.float32)
    if pieces:
        drawn = drawn * block_scale(key, dims, pieces, -0.22, 0.18)
    return jnp.clip(spiked(drawn, jax.random.fold_in(key, 3), *heavy), -reach, reach).astype(dtype)


def setup_inputs(seed: int = 0) -> dict:
    arg_keys = jax.random.split(jax.random.key(seed), 19)
    return {
        "tokens": noise_with(arg_keys[0], (TOKENS, D), 1.0, 6.0, ((0, 32),), (0, 1, 32, 2.75)),
        "segments": jax.vmap(lambda own: jnp.searchsorted(jnp.cumsum(uneven(own, max(4, SEQ_LEN // 256), SEQ_LEN, SEQ_LEN // 2, 2)), jnp.arange(SEQ_LEN), side="right"))(jax.random.split(arg_keys[1], SEQS)).reshape((SEQS, SEQ_LEN)).astype(jnp.int32),
        "cotangent": noise_with(arg_keys[2], (TOKENS, D), 1.0, 6.0, ((0, 32),), (0, 1, 32, 2.75)),
        "query_weight": gaussian(arg_keys[3], (D, D), D ** -0.5, 0.21875, ((0, 32),), jnp.float32),
        "query_bias": gaussian(arg_keys[4], (D,), 0.5, 3.0, ((0, 32),), jnp.float32),
        "key_weight": gaussian(arg_keys[5], (D, D), D ** -0.5, 0.21875, ((0, 32),), jnp.float32),
        "value_weight": gaussian(arg_keys[6], (D, D), D ** -0.5, 0.21875, ((0, 32),), jnp.float32),
        "value_bias": gaussian(arg_keys[7], (D,), 0.5, 3.0, ((0, 32),), jnp.float32),
        "mixer_weight": gaussian(arg_keys[8], (D, D), (D // 48) ** -0.5, 1.5, ((0, 32),), jnp.float32),
        "mixer_bias": gaussian(arg_keys[9], (D,), 0.3, 1.75, ((0, 32),), jnp.float32),
        "first_gain": jnp.clip(1.0 + 0.1 * jax.random.normal(arg_keys[10], (D,), jnp.float32), 0.5, 1.5),
        "first_shift": gaussian(arg_keys[11], (D,), 0.3, 1.75, ((0, 32),), jnp.float32),
        "inner_weight": gaussian(arg_keys[12], (D, FF), D ** -0.5, 0.21875, ((0, 32),), jnp.float32),
        "inner_bias": gaussian(arg_keys[13], (FF,), 0.5, 3.0, ((0, 32),), jnp.float32),
        "outer_weight": gaussian(arg_keys[14], (FF, D), (FF // 2) ** -0.5, 0.15625, ((0, 32),), jnp.float32),
        "outer_bias": gaussian(arg_keys[15], (D,), 0.3, 1.75, ((0, 32),), jnp.float32),
        "second_gain": jnp.clip(1.0 + 0.1 * jax.random.normal(arg_keys[16], (D,), jnp.float32), 0.5, 1.5),
        "second_shift": gaussian(arg_keys[17], (D,), 0.3, 1.75, ((0, 32),), jnp.float32),
    }


EPSILON = 1e-12
NEGATIVE = -1e+30
HIGHEST = lax.Precision.HIGHEST

@jax.custom_vjp
def low(v):
    return lax.optimization_barrier(v.astype(jnp.bfloat16)).astype(jnp.float32)

@jax.custom_vjp
def low_back(v):
    return v

def low_keep(v):
    return (low(v), None)

def low_pass(kept, grad):
    return (grad,)

def back_keep(v):
    return (v, None)

def back_low(kept, grad):
    return (low(grad),)
low.defvjp(low_keep, low_pass)
low_back.defvjp(back_keep, back_low)

def matmul(left, right):
    return jnp.dot(left, right, precision=HIGHEST, preferred_element_type=jnp.float32)

def normalize(hidden, gain, shift):
    centred = hidden - lax.optimization_barrier(jnp.mean(hidden, axis=-1, keepdims=True))
    variance = lax.optimization_barrier(jnp.mean(centred * centred, axis=-1, keepdims=True))
    return centred * lax.rsqrt(variance + EPSILON) * gain + shift

def layer(rows, params, segment):
    query_w, query_b, key_w, value_w, value_b, mixer_w, mixer_b, gain_one, shift_one, inner_w, inner_b, outer_w, outer_b, gain_two, shift_two = [low(piece) for piece in params]
    queries = low_back(low(matmul(rows, query_w) + query_b))
    keys = low_back(low(matmul(rows, key_w)))
    values = low_back(low(matmul(rows, value_w) + value_b))
    query_heads = queries.reshape(SEQ_LEN, HEADS, HD)
    key_heads = keys.reshape(SEQ_LEN, HEADS, HD)
    value_heads = values.reshape(SEQ_LEN, HEADS, HD)
    scores = low_back(jnp.einsum('qhd,khd->hqk', query_heads, key_heads, precision=HIGHEST) * HD ** (-0.5))
    allowed = (segment[:, None] == segment[None, :])[None]
    masked = jnp.where(allowed, scores, NEGATIVE)
    peak = lax.optimization_barrier(jnp.max(masked, axis=-1, keepdims=True))
    weights = jnp.where(allowed, jnp.exp(masked - peak), 0.0)
    probs = weights / lax.optimization_barrier(jnp.sum(weights, axis=-1, keepdims=True))
    mixed = jnp.einsum('hqk,khd->qhd', low(probs), value_heads, precision=HIGHEST).reshape(SEQ_LEN, D)
    mixed = low_back(low(mixed))
    attended = low_back(matmul(mixed, mixer_w) + mixer_b)
    first = normalize(rows + attended, gain_one, shift_one)
    inner = low_back(matmul(low(first), inner_w) + inner_b)
    active = low(jax.nn.gelu(inner, approximate=False))
    outer = low_back(matmul(active, outer_w) + outer_b)
    return normalize(first + outer, gain_two, shift_two)

def reference(tokens, segments, cotangent, query_weight, query_bias, key_weight, value_weight, value_bias, mixer_weight, mixer_bias, first_gain, first_shift, inner_weight, inner_bias, outer_weight, outer_bias, second_gain, second_shift):
    params = (query_weight, query_bias, key_weight, value_weight, value_bias, mixer_weight, mixer_bias, first_gain, first_shift, inner_weight, inner_bias, outer_weight, outer_bias, second_gain, second_shift)
    sequences = tokens.astype(jnp.float32).reshape(SEQS, SEQ_LEN, D)
    incoming = cotangent.astype(jnp.float32).reshape(SEQS, SEQ_LEN, D)

    def one_sequence(carry, inputs):
        rows, grad_rows_out, segment = inputs
        result, pullback = jax.vjp(lambda left, right: layer(left, right, segment), rows, params)
        grad_rows, grad_params = pullback(grad_rows_out)
        carry = jax.tree.map(lambda total, term: total + term, carry, grad_params)
        return (carry, (result.astype(jnp.bfloat16), grad_rows.astype(jnp.bfloat16)))
    start = tuple((jnp.zeros(piece.shape, jnp.float32) for piece in params))
    grads, (results, grad_tokens) = lax.scan(one_sequence, start, (sequences, incoming, segments))
    return (results.reshape(TOKENS, D), grad_tokens.reshape(TOKENS, D), grads[0], grads[1], grads[2], grads[3], grads[4], grads[5], grads[6], grads[7], grads[8], grads[9], grads[10], grads[11], grads[12], grads[13], grads[14])
```

```python
import functools

import jax
import jax.numpy as jnp
from jax import lax
from jax.sharding import PartitionSpec as P

HD = 64


EPSILON = 1e-12
NEGATIVE = -1e30


def product(left, right):
    return jnp.dot(left, right, preferred_element_type=jnp.float32)


def product_tn(left, right):
    return lax.dot_general(
        left, right, (((0,), (0,)), ((), ())), preferred_element_type=jnp.float32
    )


def product_nt(left, right):
    return lax.dot_general(
        left, right, (((1,), (1,)), ((), ())), preferred_element_type=jnp.float32
    )


def column_sum(values):
    return jnp.sum(values.astype(jnp.float32), axis=0)


def normalize(hidden, gain, shift):
    centred = hidden - jnp.mean(hidden, axis=-1, keepdims=True)
    scale = lax.rsqrt(jnp.mean(centred * centred, axis=-1, keepdims=True) + EPSILON)
    normed = centred * scale
    return (normed * gain + shift, normed, scale)


def normalize_back(grad_out, normed, scale, gain):
    grad_normed = grad_out * gain
    grad_hidden = scale * (
        grad_normed
        - jnp.mean(grad_normed, axis=-1, keepdims=True)
        - normed * jnp.mean(grad_normed * normed, axis=-1, keepdims=True)
    )
    return (grad_hidden, jnp.sum(grad_out * normed, axis=0), jnp.sum(grad_out, axis=0))


def attend_forward(queries, keys, values, segment):
    length, width = queries.shape
    heads = width // HD
    block = min(512, length)
    count = length // block
    scale = HD ** (-0.5)
    key_heads = keys.reshape(length, heads, HD)
    value_heads = values.reshape(length, heads, HD)
    query_blocks = queries.reshape(count, block, heads, HD)
    segment_blocks = segment.reshape(count, block)

    def one_block(inputs):
        query_block, segment_block = inputs
        scores = (
            jnp.einsum("qhd,khd->hqk", query_block, key_heads, preferred_element_type=jnp.float32)
            * scale
        )
        allowed = (segment_block[:, None] == segment[None, :])[None]
        masked = jnp.where(allowed, scores, NEGATIVE)
        peak = jnp.max(masked, axis=-1, keepdims=True)
        weights = jnp.where(allowed, jnp.exp(masked - peak), 0.0)
        total = jnp.sum(weights, axis=-1, keepdims=True)
        probs = (weights / total).astype(jnp.bfloat16)
        mixed = jnp.einsum("hqk,khd->qhd", probs, value_heads, preferred_element_type=jnp.float32)
        return (mixed.astype(jnp.bfloat16), (peak + jnp.log(total))[..., 0])

    mixed, logsum = lax.map(one_block, (query_blocks, segment_blocks))
    return (mixed.reshape(length, width), logsum)


def attend_back(queries, keys, values, segment, logsum, grad_mixed):
    length, width = queries.shape
    heads = width // HD
    block = min(512, length)
    count = length // block
    scale = HD ** (-0.5)
    key_heads = keys.reshape(length, heads, HD)
    value_heads = values.reshape(length, heads, HD)
    query_blocks = queries.reshape(count, block, heads, HD)
    grad_blocks = grad_mixed.reshape(count, block, heads, HD)
    segment_blocks = segment.reshape(count, block)

    def one_block(carry, inputs):
        key_total, value_total = carry
        query_block, segment_block, logsum_block, grad_block = inputs
        scores = (
            jnp.einsum("qhd,khd->hqk", query_block, key_heads, preferred_element_type=jnp.float32)
            * scale
        )
        allowed = (segment_block[:, None] == segment[None, :])[None]
        probs = jnp.where(allowed, jnp.exp(scores - logsum_block[..., None]), 0.0)
        grad_probs = jnp.einsum(
            "qhd,khd->hqk", grad_block, value_heads, preferred_element_type=jnp.float32
        )
        delta = jnp.sum(probs * grad_probs, axis=-1, keepdims=True)
        grad_scores = (probs * (grad_probs - delta)).astype(jnp.bfloat16)
        grad_query = (
            jnp.einsum("hqk,khd->qhd", grad_scores, key_heads, preferred_element_type=jnp.float32)
            * scale
        )
        key_total = (
            key_total
            + jnp.einsum(
                "hqk,qhd->khd", grad_scores, query_block, preferred_element_type=jnp.float32
            )
            * scale
        )
        value_total = value_total + jnp.einsum(
            "hqk,qhd->khd",
            probs.astype(jnp.bfloat16),
            grad_block,
            preferred_element_type=jnp.float32,
        )
        return ((key_total, value_total), grad_query.astype(jnp.bfloat16))

    start = jnp.zeros((length, heads, HD), jnp.float32)
    (key_total, value_total), grad_queries = lax.scan(
        one_block, (start, start), (query_blocks, segment_blocks, logsum, grad_blocks)
    )
    return (
        grad_queries.reshape(length, width),
        key_total.reshape(length, width).astype(jnp.bfloat16),
        value_total.reshape(length, width).astype(jnp.bfloat16),
    )


def hop(value, axis, bit, size):
    return lax.ppermute(value, axis, [(i, i ^ bit) for i in range(size)])


def pick(blocks, index):
    return lax.dynamic_index_in_dim(blocks, index, 0, keepdims=False)


def spread_seq(own):
    one = hop(own, "seq", 1, 4)
    three = hop(own, "seq", 3, 4)
    two = hop(three, "seq", 1, 4)
    return [own, one, two, three]


def spread_plane(blocks):
    from_x = hop(blocks, "fsdp", 2, 8)
    from_y = hop(blocks, "fsdp", 4, 8)
    far_low = hop(from_x[:2], "fsdp", 4, 8)
    far_high = hop(from_y[2:], "fsdp", 2, 8)
    parts = [[blocks], [from_x], [from_y], [far_low, far_high]]
    whole = []
    for part in parts:
        whole.append(part)
        whole.append([hop(piece, "fsdp", 1, 8) for piece in part])
    return [jnp.concatenate(part, axis=0) if len(part) > 1 else part[0] for part in whole]


def in_order(blocks, me):
    return jnp.stack([pick(blocks, j ^ me) for j in range(blocks.shape[0])])


def sum_plane(grad, me):
    theirs = jnp.stack([pick(grad, me ^ (2 * k + 1)) for k in range(4)])
    mine = [pick(grad, me ^ (2 * k)) for k in range(4)]
    got = hop(theirs, "fsdp", 1, 8)
    total = [mine[k] + got[k] for k in range(4)]
    half = total[3].shape[0] // 2
    far_y = hop(total[3][:half], "fsdp", 4, 8)
    far_x = hop(total[3][half:], "fsdp", 2, 8)
    to_x = jnp.concatenate([total[1][:half] + far_y, total[1][half:]], axis=0)
    to_y = jnp.concatenate([total[2][:half], total[2][half:] + far_x], axis=0)
    near_x = hop(to_x, "fsdp", 2, 8)
    near_y = hop(to_y, "fsdp", 4, 8)
    return total[0] + near_x + near_y


def sum_seq(blocks, z):
    far = hop(pick(blocks, z ^ 2), "seq", 1, 4)
    near = hop(pick(blocks, z ^ 1), "seq", 1, 4)
    last = hop(pick(blocks, z ^ 3) + far, "seq", 3, 4)
    return (
        pick(blocks, z).astype(jnp.float32)
        + near.astype(jnp.float32)
        + last.astype(jnp.float32)
    )


def gather_rows(own, fast, f, z):
    if not fast:
        return lax.all_gather(own, ("fsdp", "seq"), axis=0, tiled=True)
    rows, width = own.shape
    pieces = jnp.stack(spread_plane(jnp.stack(spread_seq(own))))
    pieces = in_order(pieces, f)
    pieces = jnp.stack([pick(pieces.swapaxes(0, 1), j ^ z) for j in range(4)], axis=1)
    return pieces.reshape(32 * rows, width)


def reduce_rows(grad, fast, f, z):
    if not fast:
        return lax.psum_scatter(
            grad.astype(jnp.float32), ("fsdp", "seq"), scatter_dimension=0, tiled=True
        )
    rows = grad.shape[0] // 32
    mine = sum_plane(grad.reshape(8, 4, rows, grad.shape[1]), f)
    return sum_seq(mine, z)


def on_device(
    sizes,
    tokens,
    segments,
    cotangent,
    query_weight,
    query_bias,
    key_weight,
    value_weight,
    value_bias,
    mixer_weight,
    mixer_bias,
    first_gain,
    first_shift,
    inner_weight,
    inner_bias,
    outer_weight,
    outer_bias,
    second_gain,
    second_shift,
):
    nf, nz = sizes
    fast = (nf, nz) == (8, 4)
    f, z = lax.axis_index("fsdp"), lax.axis_index("seq")
    low = jnp.bfloat16
    share, width = query_weight.shape
    wide = inner_weight.shape[1]
    cut = width // nz
    ratio = wide // width
    small = jnp.stack(
        [
            piece.astype(low)
            for piece in (
                query_bias,
                value_bias,
                mixer_bias,
                first_gain,
                first_shift,
                outer_bias,
                second_gain,
                second_shift,
            )
        ]
        + list(inner_bias.astype(low).reshape(ratio, share)),
        axis=1,
    )
    heads_of = [
        piece.astype(low).reshape(share, nz, cut) for piece in (query_weight, key_weight, value_weight)
    ]

    if fast:
        pieces = jnp.stack(spread_seq(tokens))
        rows_all = in_order(pieces, z).reshape(-1, width)
    else:
        rows_all = lax.all_gather(tokens, "seq", axis=0, tiled=True)

    def message(target):
        return jnp.concatenate(
            [lax.dynamic_index_in_dim(piece, target, 1, keepdims=False) for piece in heads_of] + [small],
            axis=1,
        )

    if fast:
        got = [message(z)] + [hop(message(z ^ k), "seq", k, 4) for k in (1, 2, 3)]
        got = jnp.stack(spread_plane(jnp.stack(got)))
        got = in_order(got, f)
        got = jnp.stack([pick(got.swapaxes(0, 1), j ^ z) for j in range(4)], axis=1)
        heads_full = got.reshape(width, -1)
    else:
        packed = jnp.concatenate(
            [piece.astype(low) for piece in (query_weight, key_weight, value_weight)] + [small], axis=1
        )
        packed = lax.all_gather(packed, ("fsdp", "seq"), axis=0, tiled=True)
        heads_full = jnp.concatenate(
            [
                lax.dynamic_slice_in_dim(packed, k * width + z * cut, cut, axis=1)
                for k in range(3)
            ]
            + [packed[:, 3 * width :]],
            axis=1,
        )
    small_full = heads_full[:, 3 * cut :].astype(jnp.float32).T
    (qbias, vbias, mbias, gain_one, shift_one, obias, gain_two, shift_two) = [
        small_full[k] for k in range(8)
    ]
    ibias = (
        small_full[8:].reshape(ratio, nf * nz, share).swapaxes(0, 1).reshape(wide)
    )
    qbias = lax.dynamic_slice_in_dim(qbias, z * cut, cut)
    vbias = lax.dynamic_slice_in_dim(vbias, z * cut, cut)

    packed = jnp.concatenate(
        [mixer_weight.astype(low)]
        + [inner_weight[:, k * width : (k + 1) * width].astype(low) for k in range(ratio)],
        axis=0,
    )
    packed = gather_rows(packed, fast, f, z).reshape(nf * nz, 1 + ratio, share, width)
    mixer_full = packed[:, 0].reshape(width, width)
    inner_full = jnp.concatenate(
        [packed[:, 1 + k].reshape(width, width) for k in range(ratio)], axis=1
    )
    outer_full = gather_rows(outer_weight.astype(low), fast, f, z)

    projected = product(rows_all, heads_full[:, : 3 * cut])
    query_heads = (projected[:, :cut] + qbias).astype(low)
    key_heads = projected[:, cut : 2 * cut].astype(low)
    value_heads = (projected[:, 2 * cut :] + vbias).astype(low)
    segment = segments[0]
    mixed_heads, logsum = attend_forward(query_heads, key_heads, value_heads, segment)
    mixed_rows = lax.all_to_all(mixed_heads, "seq", split_axis=0, concat_axis=1, tiled=True)
    attended = product(mixed_rows, mixer_full) + mbias
    first_out, first_normed, first_scale = normalize(
        tokens.astype(jnp.float32) + attended, gain_one, shift_one
    )
    first_low = first_out.astype(low)
    inner_pre = product(first_low, inner_full) + ibias
    active, gelu_back = jax.vjp(lambda value: jax.nn.gelu(value, approximate=False), inner_pre)
    active_low = active.astype(low)
    outer = product(active_low, outer_full) + obias
    result, second_normed, second_scale = normalize(first_out + outer, gain_two, shift_two)
    grad_second, grad_gain_two, grad_shift_two = normalize_back(
        cotangent.astype(jnp.float32), second_normed, second_scale, gain_two
    )
    grad_outer = grad_second.astype(low)
    grad_outer_weight = product_tn(active_low, grad_outer).astype(low)
    grad_outer_bias = column_sum(grad_outer)
    outer_sum = reduce_rows(grad_outer_weight, fast, f, z)
    grad_inner = gelu_back(product_nt(grad_outer, outer_full))[0].astype(low)
    grad_inner_weight = product_tn(first_low, grad_inner).astype(low)
    grad_inner_bias = column_sum(grad_inner)
    grad_first_out = grad_second + product_nt(grad_inner, inner_full)
    grad_residual, grad_gain_one, grad_shift_one = normalize_back(
        grad_first_out, first_normed, first_scale, gain_one
    )
    grad_attended = grad_residual.astype(low)
    grad_mixer_weight = product_tn(mixed_rows, grad_attended).astype(low)
    grad_mixer_bias = column_sum(grad_attended)
    packed = jnp.concatenate(
        [grad_mixer_weight.reshape(nf * nz, 1, share, width)]
        + [
            grad_inner_weight[:, k * width : (k + 1) * width].reshape(nf * nz, 1, share, width)
            for k in range(ratio)
        ],
        axis=1,
    ).reshape(-1, width)
    packed_sum = reduce_rows(packed, fast, f, z)
    mixer_sum = packed_sum[:share]
    inner_sum = jnp.concatenate(
        [packed_sum[(1 + k) * share : (2 + k) * share] for k in range(ratio)], axis=1
    )
    grad_mixed = product_nt(grad_attended, mixer_full).astype(low)
    grad_mixed_heads = lax.all_to_all(grad_mixed, "seq", split_axis=1, concat_axis=0, tiled=True)
    grad_query_heads, grad_key_heads, grad_value_heads = attend_back(
        query_heads, key_heads, value_heads, segment, logsum, grad_mixed_heads
    )
    grads = jnp.concatenate([grad_query_heads, grad_key_heads, grad_value_heads], axis=1)
    heads_grad = product_tn(rows_all, grads).astype(low)
    zero = jnp.zeros((width,), jnp.float32)
    small_grad = jnp.stack(
        [
            lax.dynamic_update_slice_in_dim(zero, column_sum(grad_query_heads), z * cut, 0),
            lax.dynamic_update_slice_in_dim(zero, column_sum(grad_value_heads), z * cut, 0),
            grad_mixer_bias,
            grad_gain_one,
            grad_shift_one,
            grad_outer_bias,
            grad_gain_two,
            grad_shift_two,
        ]
        + list(grad_inner_bias.reshape(nf * nz, ratio, share).swapaxes(0, 1).reshape(ratio, width)),
        axis=1,
    ).astype(low)
    heads_grad = jnp.concatenate([heads_grad, small_grad], axis=1)
    if fast:
        mine = sum_plane(heads_grad.reshape(8, 4, share, -1), f)
        parts = [pick(mine, z)] + [hop(pick(mine, z ^ k), "seq", k, 4) for k in (1, 2, 3)]
        parts = in_order(jnp.stack(parts), z)
    else:
        mine = lax.psum_scatter(heads_grad, "fsdp", scatter_dimension=0, tiled=True)
        parts = lax.all_to_all(
            mine.reshape(nz, share, -1), "seq", split_axis=0, concat_axis=0, tiled=True
        )
    parts = parts.astype(jnp.float32)
    projections = [
        jnp.concatenate([parts[j, :, k * cut : (k + 1) * cut] for j in range(nz)], axis=1)
        for k in range(3)
    ]
    small_sum = jnp.sum(parts[:, :, 3 * cut :], axis=0).T
    back_rows = product_nt(grads, heads_full[:, : 3 * cut]).astype(low).reshape(nz, -1, width)
    if fast:
        back = sum_seq(back_rows, z)
    else:
        back = lax.psum_scatter(back_rows, "seq", scatter_dimension=0, tiled=True)[0]
    grad_tokens = grad_residual + back
    return (
        result.astype(low),
        grad_tokens.astype(low),
        projections[0],
        small_sum[0],
        projections[1],
        projections[2],
        small_sum[1],
        mixer_sum,
        small_sum[2],
        small_sum[3],
        small_sum[4],
        inner_sum,
        small_sum[8:].reshape(-1),
        outer_sum,
        small_sum[5],
        small_sum[6],
        small_sum[7],
    )


def solution(mesh):
    placed = (
        P(("fsdp", "seq"), None),
        P("fsdp", None),
        P(("fsdp", "seq"), None),
        P(("fsdp", "seq"), None),
        P(("fsdp", "seq")),
        P(("fsdp", "seq"), None),
        P(("fsdp", "seq"), None),
        P(("fsdp", "seq")),
        P(("fsdp", "seq"), None),
        P(("fsdp", "seq")),
        P(("fsdp", "seq")),
        P(("fsdp", "seq")),
        P(("fsdp", "seq"), None),
        P(("fsdp", "seq")),
        P(("fsdp", "seq"), None),
        P(("fsdp", "seq")),
        P(("fsdp", "seq")),
        P(("fsdp", "seq")),
    )
    sizes = (mesh.shape["fsdp"], mesh.shape["seq"])
    return jax.shard_map(
        functools.partial(on_device, sizes),
        mesh=mesh,
        in_specs=placed,
        out_specs=(
            P(("fsdp", "seq"), None),
            P(("fsdp", "seq"), None),
            P(("fsdp", "seq"), None),
            P(("fsdp", "seq")),
            P(("fsdp", "seq"), None),
            P(("fsdp", "seq"), None),
            P(("fsdp", "seq")),
            P(("fsdp", "seq"), None),
            P(("fsdp", "seq")),
            P(("fsdp", "seq")),
            P(("fsdp", "seq")),
            P(("fsdp", "seq"), None),
            P(("fsdp", "seq")),
            P(("fsdp", "seq"), None),
            P(("fsdp", "seq")),
            P(("fsdp", "seq")),
            P(("fsdp", "seq")),
        ),
        check_vma=False,
    )
```

```python
import functools
import math

import jax
import jax.numpy as jnp
from jax import lax
from jax.experimental import pallas as pl
from jax.experimental.pallas import tpu as pltpu
from jax.sharding import PartitionSpec as P

HD = 64


EPSILON = 1e-12
NEGATIVE = -1e30


def product(left, right):
    return jnp.dot(left, right, preferred_element_type=jnp.float32)


def product_tn(left, right):
    return lax.dot_general(
        left, right, (((0,), (0,)), ((), ())), preferred_element_type=jnp.float32
    )


def product_nt(left, right):
    return lax.dot_general(
        left, right, (((1,), (1,)), ((), ())), preferred_element_type=jnp.float32
    )


def column_sum(values):
    return jnp.sum(values.astype(jnp.float32), axis=0)


def normalize(hidden, gain, shift):
    centred = hidden - jnp.mean(hidden, axis=-1, keepdims=True)
    scale = lax.rsqrt(jnp.mean(centred * centred, axis=-1, keepdims=True) + EPSILON)
    normed = centred * scale
    return (normed * gain + shift, normed, scale)


def normalize_back(grad_out, normed, scale, gain):
    grad_normed = grad_out * gain
    grad_hidden = scale * (
        grad_normed
        - jnp.mean(grad_normed, axis=-1, keepdims=True)
        - normed * jnp.mean(grad_normed * normed, axis=-1, keepdims=True)
    )
    return (grad_hidden, jnp.sum(grad_out * normed, axis=0), jnp.sum(grad_out, axis=0))


def attend_forward(queries, keys, values, segment):
    length, width = queries.shape
    heads = width // HD
    block = min(512, length)
    count = length // block
    scale = HD ** (-0.5)
    key_heads = keys.reshape(length, heads, HD)
    value_heads = values.reshape(length, heads, HD)
    query_blocks = queries.reshape(count, block, heads, HD)
    segment_blocks = segment.reshape(count, block)

    def one_block(inputs):
        query_block, segment_block = inputs
        scores = (
            jnp.einsum("qhd,khd->hqk", query_block, key_heads, preferred_element_type=jnp.float32)
            * scale
        )
        allowed = (segment_block[:, None] == segment[None, :])[None]
        masked = jnp.where(allowed, scores, NEGATIVE)
        peak = jnp.max(masked, axis=-1, keepdims=True)
        weights = jnp.where(allowed, jnp.exp(masked - peak), 0.0)
        total = jnp.sum(weights, axis=-1, keepdims=True)
        probs = (weights / total).astype(jnp.bfloat16)
        mixed = jnp.einsum("hqk,khd->qhd", probs, value_heads, preferred_element_type=jnp.float32)
        return (mixed.astype(jnp.bfloat16), (peak + jnp.log(total))[..., 0])

    mixed, logsum = lax.map(one_block, (query_blocks, segment_blocks))
    return (mixed.reshape(length, width), logsum)


def attend_back(queries, keys, values, segment, logsum, grad_mixed):
    length, width = queries.shape
    heads = width // HD
    block = min(512, length)
    count = length // block
    scale = HD ** (-0.5)
    key_heads = keys.reshape(length, heads, HD)
    value_heads = values.reshape(length, heads, HD)
    query_blocks = queries.reshape(count, block, heads, HD)
    grad_blocks = grad_mixed.reshape(count, block, heads, HD)
    segment_blocks = segment.reshape(count, block)

    def one_block(carry, inputs):
        key_total, value_total = carry
        query_block, segment_block, logsum_block, grad_block = inputs
        scores = (
            jnp.einsum("qhd,khd->hqk", query_block, key_heads, preferred_element_type=jnp.float32)
            * scale
        )
        allowed = (segment_block[:, None] == segment[None, :])[None]
        probs = jnp.where(allowed, jnp.exp(scores - logsum_block[..., None]), 0.0)
        grad_probs = jnp.einsum(
            "qhd,khd->hqk", grad_block, value_heads, preferred_element_type=jnp.float32
        )
        delta = jnp.sum(probs * grad_probs, axis=-1, keepdims=True)
        grad_scores = (probs * (grad_probs - delta)).astype(jnp.bfloat16)
        grad_query = (
            jnp.einsum("hqk,khd->qhd", grad_scores, key_heads, preferred_element_type=jnp.float32)
            * scale
        )
        key_total = (
            key_total
            + jnp.einsum(
                "hqk,qhd->khd", grad_scores, query_block, preferred_element_type=jnp.float32
            )
            * scale
        )
        value_total = value_total + jnp.einsum(
            "hqk,qhd->khd",
            probs.astype(jnp.bfloat16),
            grad_block,
            preferred_element_type=jnp.float32,
        )
        return ((key_total, value_total), grad_query.astype(jnp.bfloat16))

    start = jnp.zeros((length, heads, HD), jnp.float32)
    (key_total, value_total), grad_queries = lax.scan(
        one_block, (start, start), (query_blocks, segment_blocks, logsum, grad_blocks)
    )
    return (
        grad_queries.reshape(length, width),
        key_total.reshape(length, width).astype(jnp.bfloat16),
        value_total.reshape(length, width).astype(jnp.bfloat16),
    )


def hop(value, axis, bit, size):
    return lax.ppermute(value, axis, [(i, i ^ bit) for i in range(size)])


def pick(blocks, index):
    return lax.dynamic_index_in_dim(blocks, index, 0, keepdims=False)


def spread_seq(own):
    one = hop(own, "seq", 1, 4)
    three = hop(own, "seq", 3, 4)
    two = hop(three, "seq", 1, 4)
    return [own, one, two, three]


def spread_plane(blocks):
    from_x = hop(blocks, "fsdp", 2, 8)
    from_y = hop(blocks, "fsdp", 4, 8)
    far_low = hop(from_x[:2], "fsdp", 4, 8)
    far_high = hop(from_y[2:], "fsdp", 2, 8)
    out = []
    for part in ([blocks], [from_x], [from_y], [far_low, far_high]):
        out += part + [hop(piece, "fsdp", 1, 8) for piece in part]
    return out


def after(values):
    return lax.optimization_barrier(values)


def sum_far(got, mine):
    half = mine.shape[1] // 2
    far_y = hop(mine[3, :half] + got[3, :half], "fsdp", 4, 8)
    far_x = hop(mine[3, half:] + got[3, half:], "fsdp", 2, 8)
    return far_y, far_x


def sum_near(got, mine, far_y, far_x):
    half = mine.shape[1] // 2
    to_x = jnp.concatenate([mine[1, :half] + got[1, :half] + far_y, mine[1, half:] + got[1, half:]], axis=0)
    to_y = jnp.concatenate([mine[2, :half] + got[2, :half], mine[2, half:] + got[2, half:] + far_x], axis=0)
    return hop(to_x, "fsdp", 2, 8), hop(to_y, "fsdp", 4, 8)


def sum_plane(theirs, mine):
    got = hop(theirs, "fsdp", 1, 8)
    near_x, near_y = sum_near(got, mine, *sum_far(got, mine))
    return mine[0] + got[0] + near_x + near_y


def sum_seq(two, one, three, own):
    far = hop(two, "seq", 1, 4)
    near = hop(one, "seq", 1, 4)
    last = hop(three + far, "seq", 3, 4)
    return own.astype(jnp.float32) + near.astype(jnp.float32) + last.astype(jnp.float32)


def sum_place(total, z):
    return sum_seq(pick(total, z ^ 2), pick(total, z ^ 1), pick(total, z ^ 3), pick(total, z))


def xpose(value):
    return jnp.transpose(value)


def place(pieces, into, sems, me_ref, rows):
    copies = []
    for kf, group in enumerate(pieces):
        for kz in range(4):
            ref, at = group[kz * len(group) // 4], kz % (4 // len(group))
            to = ((me_ref[0] ^ kf) * 4 + (me_ref[1] ^ kz)) * rows
            to = pl.multiple_of(to, 8)
            target = into.at[:, pl.ds(to, rows)] if len(into.shape) == 3 else into.at[pl.ds(to, rows)]
            copies.append(pltpu.make_async_copy(ref.at[at], target, sems.at[kf * 4 + kz]))
    return copies


def regroup(refs):
    out, at = [], 0
    for kf in range(8):
        n = 2 if kf >= 6 else 1
        out.append(refs[at : at + n])
        at += n
    return out


def dot(left, right, dims=((1,), (0,))):
    return lax.dot_general(left, right, (dims, ((), ())), preferred_element_type=jnp.float32)


NT = ((1,), (1,))
TN = ((0,), (0,))


def prepare_kernel(me_ref, *refs):
    pieces = regroup(refs[:10])
    wt_out, small_out, ib_out, bias_out, w, stack, sems = refs[10:]
    low, z = jnp.bfloat16, me_ref[1]
    copies = place(pieces, w, sems, me_ref, 24)
    for copy in copies:
        copy.start()
    for copy in copies:
        copy.wait()
    wt = xpose(w[...])
    wt_out[...] = wt
    small_out[...] = wt[576:592].astype(jnp.float32)
    for g in range(8):
        stack[8 * g : 8 * g + 8] = small_out[8:16, 96 * g : 96 * g + 96]
    heap = stack[...].astype(low)
    line = lax.broadcasted_iota(jnp.int32, (64, 384), 0) & 7
    spread = jnp.zeros((64, 384), jnp.float32)
    for c in range(4):
        spread = spread + jnp.where(line == c, dot(heap, shares(c)), 0.0)
    for g in range(8):
        ib_out[:, 384 * g : 384 * g + 384] = total_rows(spread[8 * g : 8 * g + 8])
    bias = w[pl.ds(pl.multiple_of(z * 192, 64), 192), 512:640].astype(jnp.float32)
    bias_out[0] = jnp.broadcast_to(bias[:, 64:65], (192, 128))
    bias_out[1] = jnp.broadcast_to(bias[:, 65:66], (192, 128))


def turn_kernel(me_ref, *refs):
    xs, xt_out, xt = refs[:4], refs[4], refs[5]
    for k in range(4):
        xt[:, 256 * k : 256 * k + 256] = xpose(xs[k][...])
    for kf in range(8):
        xt_out[96 * kf : 96 * kf + 96] = xt[pl.ds(pl.multiple_of((me_ref[0] ^ kf) * 96, 32), 96)]


def attend_kernel(*refs):
    xs, refs = refs[:4], refs[4:]
    wt, bias, seg_row, seg_col, refs = refs[0], refs[1], refs[2], refs[3], refs[4:]
    q_out, k_out, v_out, *m_out = refs[:7]
    lse_out, keys, mixed = refs[7:]
    low = jnp.bfloat16
    for k in range(4):
        at = slice(256 * k, 256 * k + 256)
        qkv = dot(wt[:576], xs[k][...], NT)
        query = (qkv[:192] + bias[0, :, 0:1]).astype(low)
        query = (query.astype(jnp.float32) * HD**-0.5).astype(low)
        key = qkv[192:384].astype(low)
        value = (qkv[384:] + bias[1, :, 0:1]).astype(low)
        for h in range(3):
            rows = slice(64 * h, 64 * h + 64)
            q_out[h, :, at] = query[rows]
            k_out[h, :, at] = key[rows]
            v_out[h, :, at] = value[rows]
            keys[h, at] = xpose(key[rows])

    def step(i, carry):
        h, b = lax.shift_right_logical(i, 2), i & 3
        at = pl.ds(pl.multiple_of(b * 256, 256), 256)
        scores = dot(keys[h], q_out[h, :, at])
        column = seg_col[...]
        allowed = jnp.concatenate([column, column], axis=1) == seg_row[:, at]
        scores = jnp.where(allowed, scores, NEGATIVE)
        peak = jnp.max(scores, axis=0, keepdims=True)
        weights = jnp.exp(scores - peak)
        total = jnp.sum(weights, axis=0, keepdims=True)
        probs = (weights * (1.0 / total)).astype(low)
        mixed[b, h] = dot(v_out[h], probs).astype(low)
        lse_out[h, :, at] = peak + jnp.log(total)
        return carry

    lax.fori_loop(0, 12, step, 0)
    for k in range(4):
        for h in range(3):
            m_out[k][64 * h : 64 * h + 64] = mixed[k, h]


VM = pl.BlockSpec(memory_space=pltpu.VMEM)
ANY = pl.BlockSpec(memory_space=pl.ANY)
SM = pl.BlockSpec(memory_space=pltpu.SMEM)


def shape(*dims, dtype=jnp.bfloat16):
    return jax.ShapeDtypeStruct(dims, dtype)


def cost(flops, moved, powers=0):
    return pl.CostEstimate(flops=1, bytes_accessed=1, transcendentals=0)


def prepare_call(me, pieces):
    f32 = jnp.float32
    outs = [
        shape(640, 768),
        shape(16, 768, dtype=f32),
        shape(1, 3072, dtype=f32),
        shape(2, 192, 128, dtype=f32),
    ]
    return pl.pallas_call(
        prepare_kernel,
        out_shape=outs,
        in_specs=[SM] + [ANY] * 10,
        out_specs=[VM] * len(outs),
        scratch_shapes=[
            pltpu.VMEM((768, 640), jnp.bfloat16),
            pltpu.VMEM((64, 96), f32),
            pltpu.SemaphoreType.DMA((32,)),
        ],
        cost_estimate=cost(100_000_000, 4_000_000),
        name="prepare",
    )(me, *pieces)


def turn_call(me, xs):
    return pl.pallas_call(
        turn_kernel,
        out_shape=shape(768, 1024),
        in_specs=[SM] + [VM] * 4,
        out_specs=VM,
        scratch_shapes=[pltpu.VMEM((768, 1024), jnp.bfloat16)],
        cost_estimate=cost(100_000_000, 3_200_000),
        name="turn",
    )(me, *xs)


def attend_call(xs, wt, bias, seg_row, seg_col):
    outs = [shape(3, 64, 1024)] * 3 + [shape(192, 256)] * 4 + [shape(3, 1, 1024, dtype=jnp.float32)]
    return pl.pallas_call(
        attend_kernel,
        out_shape=outs,
        in_specs=[VM] * 8,
        out_specs=[VM] * len(outs),
        scratch_shapes=[
            pltpu.VMEM((3, 1024, 64), jnp.bfloat16),
            pltpu.VMEM((4, 3, 64, 256), jnp.bfloat16),
        ],
        cost_estimate=cost(6_000_000_000, 10_000_000, 3_145_728),
        name="attend",
    )(*xs, wt, bias, seg_row, seg_col)


def pack_kernel(me_ref, vectors, segments, query, key, value, mixer, inner, outer, *refs):
    messages, both, outs, seg_row, seg_col, rows = refs[:4], refs[4], refs[5], refs[6], refs[7], refs[8]
    low, z = jnp.bfloat16, me_ref[1]
    rows[...] = jnp.zeros_like(rows)
    rows[0:12, 0:24] = vectors[...]
    small = xpose(rows[...])[:24, :64]
    parts = []
    for j in range(4):
        at = slice(192 * j, 192 * j + 192)
        parts.append(jnp.concatenate([query[:, at], key[:, at], value[:, at], small], axis=1))
    for k in range(4):
        part = parts[3]
        for j in range(3):
            part = jnp.where((z ^ k) == j, parts[j], part)
        messages[k][...] = part.astype(low)
    both[0] = mixer[...].astype(low)
    for c in range(4):
        both[1 + c] = inner[:, 768 * c : 768 * c + 768].astype(low)
    outs[...] = outer[...].astype(low)
    for k in range(4):
        at = slice(256 * k, 256 * k + 256)
        row = segments[:, pl.ds(pl.multiple_of((z ^ k) * 256, 256), 256)].astype(jnp.float32)
        seg_row[:, at] = row
        seg_col[at] = xpose(jnp.broadcast_to(row, (128, 256)))


def pack_call(me, vectors, segments, *weights):
    f32 = jnp.float32
    outs = [shape(24, 640)] * 4 + [
        shape(5, 24, 768),
        shape(96, 768),
        shape(1, 1024, dtype=f32),
        shape(1024, 128, dtype=f32),
    ]
    return pl.pallas_call(
        pack_kernel,
        out_shape=outs,
        in_specs=[SM] + [VM] * 8,
        out_specs=[VM] * len(outs),
        scratch_shapes=[pltpu.VMEM((128, 128), f32)],
        cost_estimate=cost(1, 1),
        name="pack",
    )(me, vectors, segments, *weights)


def shares(c):
    row = lax.broadcasted_iota(jnp.int32, (96, 384), 0)
    column = lax.broadcasted_iota(jnp.int32, (96, 384), 1)
    where = row + 72 * ((row >= 24).astype(jnp.int32) + (row >= 48) + (row >= 72)) + 24 * c
    return (column == where).astype(jnp.float32).astype(jnp.bfloat16)


def centre(hidden):
    centred = hidden - jnp.mean(hidden, axis=-1, keepdims=True)
    scale = lax.rsqrt(jnp.mean(centred * centred, axis=-1, keepdims=True) + EPSILON)
    return centred * scale, scale


def centre_back(grad_normed, normed, scale):
    return scale * (
        grad_normed
        - jnp.mean(grad_normed, axis=-1, keepdims=True)
        - normed * jnp.mean(grad_normed * normed, axis=-1, keepdims=True)
    )


def total_rows(value):
    return jnp.sum(value, axis=0, keepdims=True)


def feed_kernel(me_ref, *refs):
    ms, refs = refs[:4], refs[4:]
    tokens, cotangent, small, ibias, refs = refs[0], refs[1], refs[2], refs[3], refs[4:]
    pieces, outers, refs = regroup(refs[:10]), regroup(refs[10:20]), refs[20:]
    result, slope_out, first_out, normed_out, scale_out, second_out, gouter_out, sums, theirs, mine = refs[:10]
    wmi, wo, active, sems, osems = refs[10:]
    low, f32, f, z = jnp.bfloat16, jnp.float32, me_ref[0], me_ref[1]
    copies = place(pieces, wmi, sems, me_ref, 24)
    ocopies = place(outers, wo, osems, me_ref, 96)
    for copy in copies + ocopies:
        copy.start()
    for copy in copies:
        copy.wait()
    attended = small[2:3]
    for k in range(4):
        rows = wmi[0, pl.ds(pl.multiple_of((z ^ k) * 192, 64), 192)]
        attended = attended + dot(ms[k][...], rows, TN)
    normed, scale = centre(tokens[...].astype(f32) + attended)
    normed_out[...] = normed
    scale_out[...] = jnp.broadcast_to(scale, (256, 128))
    first = normed * small[3:4] + small[4:5]
    first_low = first.astype(low)
    first_out[...] = first_low
    for copy in ocopies:
        copy.wait()
    outer = small[5:6]
    for c in range(4):
        at = slice(768 * c, 768 * c + 768)
        inner = dot(first_low, wmi[1 + c]) + ibias[:, at]
        half = 0.5 + 0.5 * lax.erf(inner * (0.5**0.5))
        slope_out[:, at] = half + inner * jnp.exp(-0.5 * inner * inner) * ((2.0 * math.pi) ** -0.5)
        act = (inner * half).astype(low)
        active[:, at] = act
        outer = outer + dot(act, wo[at])
    normed, scale = centre(first + outer)
    result[...] = (normed * small[6:7] + small[7:8]).astype(low)
    grad = cotangent[...].astype(f32)
    second = centre_back(grad * small[6:7], normed, scale)
    second_out[...] = second
    gouter = second.astype(low)
    gouter_out[...] = gouter
    sums[0:1] = total_rows(gouter.astype(f32))
    sums[1:2] = total_rows(grad * normed)
    sums[2:3] = total_rows(grad)
    sums[3:8] = jnp.zeros((5, 768), f32)

    def step(kp, carry):
        for kc, out in ((1, theirs), (0, mine)):
            at = pl.ds(pl.multiple_of((f ^ (2 * kp + kc)) * 384, 128), 384)
            out[kp] = dot(active[:, at], gouter_out[...], TN).astype(low)
        return carry

    lax.fori_loop(0, 4, step, 0)


def feed_call(me, ms, tokens, cotangent, small, ibias, pieces, outers):
    f32 = jnp.float32
    outs = [
        shape(256, 768),
        shape(256, 3072, dtype=f32),
        shape(256, 768),
        shape(256, 768, dtype=f32),
        shape(256, 128, dtype=f32),
        shape(256, 768, dtype=f32),
        shape(256, 768),
        shape(8, 768, dtype=f32),
        shape(4, 384, 768),
        shape(4, 384, 768),
    ]
    return pl.pallas_call(
        feed_kernel,
        out_shape=outs,
        in_specs=[SM] + [VM] * 8 + [ANY] * 20,
        out_specs=[VM] * len(outs),
        scratch_shapes=[
            pltpu.VMEM((5, 768, 768), jnp.bfloat16),
            pltpu.VMEM((3072, 768), jnp.bfloat16),
            pltpu.VMEM((256, 3072), jnp.bfloat16),
            pltpu.SemaphoreType.DMA((32,)),
            pltpu.SemaphoreType.DMA((32,)),
        ],
        cost_estimate=cost(1, 1),
        name="feed",
    )(me, *ms, tokens, cotangent, small, ibias, *pieces, *outers)


def feed_back_kernel(me_ref, *refs):
    small, slope, normed_ref, scale_ref, second, gouter, refs = *refs[:6], refs[6:]
    pieces, outers, refs = regroup(refs[:10]), regroup(refs[10:20]), refs[20:]
    residual, sums, isums, gin, d0, d1, d2, d3 = refs[:8]
    wmi, wo, sems, osems = refs[8:]
    low, f32, z = jnp.bfloat16, jnp.float32, me_ref[1]
    copies = place(pieces, wmi, sems, me_ref, 24)
    ocopies = place(outers, wo, osems, me_ref, 96)
    for copy in ocopies + copies:
        copy.start()
    for copy in ocopies:
        copy.wait()
    for c in range(4):
        at = slice(768 * c, 768 * c + 768)
        inner = (dot(gouter[...], wo[at], NT) * slope[:, at]).astype(low)
        gin[:, at] = inner
        isums[:, at] = total_rows(inner.astype(f32))
    for copy in copies:
        copy.wait()
    first = second[...]
    for c in range(4):
        at = slice(768 * c, 768 * c + 768)
        first = first + dot(gin[:, at], wmi[1 + c], NT)
    normed = normed_ref[...]
    grad = centre_back(first * small[3:4], normed, scale_ref[:, 0:1])
    residual[...] = grad
    sums[0:1] = total_rows(grad.astype(low).astype(f32))
    sums[1:2] = total_rows(first * normed)
    sums[2:3] = total_rows(first)
    sums[3:8] = jnp.zeros((5, 768), f32)
    attended = grad.astype(low)
    for k, out in enumerate((d0, d1, d2, d3)):
        rows = wmi[0, pl.ds(pl.multiple_of((z ^ k) * 192, 64), 192)]
        out[...] = dot(rows, attended, NT).astype(low)


def feed_back_call(me, small, slope, normed, scale, second, gouter, pieces, outers):
    f32 = jnp.float32
    outs = [
        shape(256, 768, dtype=f32),
        shape(8, 768, dtype=f32),
        shape(1, 3072, dtype=f32),
        shape(256, 3072),
    ] + [shape(192, 256)] * 4
    return pl.pallas_call(
        feed_back_kernel,
        out_shape=outs,
        in_specs=[SM] + [VM] * 6 + [ANY] * 20,
        out_specs=[VM] * len(outs),
        scratch_shapes=[
            pltpu.VMEM((5, 768, 768), jnp.bfloat16),
            pltpu.VMEM((3072, 768), jnp.bfloat16),
            pltpu.SemaphoreType.DMA((32,)),
            pltpu.SemaphoreType.DMA((32,)),
        ],
        cost_estimate=cost(8_000_000_000, 25_000_000),
        name="feed_back",
    )(me, small, slope, normed, scale, second, gouter, *pieces, *outers)


def feed_grad_kernel(me_ref, *refs):
    ms, first_low, gin, residual, theirs, mine, left, canon = refs[:4], *refs[4:]
    low, f, z = jnp.bfloat16, me_ref[0], me_ref[1]

    def order():
        for kf in range(8):
            left[96 * kf : 96 * kf + 96] = canon[pl.ds(pl.multiple_of((f ^ kf) * 96, 32), 96)]

    def spread(value, entry):
        value = value.astype(low)
        for kf in range(8):
            out = theirs if kf % 2 else mine
            for zz in range(4):
                out[kf // 2, zz, entry] = value[96 * kf + 24 * zz : 96 * kf + 24 * zz + 24]

    canon[...] = xpose(first_low[...])
    order()
    for c in range(4):
        spread(dot(left[...], gin[:, 768 * c : 768 * c + 768]), 1 + c)
    for k in range(4):
        canon[pl.ds(pl.multiple_of((z ^ k) * 192, 64), 192)] = ms[k][...]
    order()
    spread(dot(left[...], residual[...].astype(low)), 0)


def feed_grad_call(me, ms, first_low, gin, residual):
    return pl.pallas_call(
        feed_grad_kernel,
        out_shape=[shape(4, 4, 5, 24, 768)] * 2,
        in_specs=[SM] + [VM] * 7,
        out_specs=[VM] * 2,
        scratch_shapes=[pltpu.VMEM((768, 256), jnp.bfloat16)] * 2,
        cost_estimate=cost(4_000_000_000, 10_000_000),
        name="feed_grad",
    )(me, *ms, first_low, gin, residual)


def attend_back_kernel(*refs):
    ds, refs = refs[:4], refs[4:]
    q_ref, k_ref, v_ref, lse, seg_row, seg_col, all_rows = refs[:7]
    keys, values, gout, gk, gv = refs[7:]
    low = jnp.bfloat16
    for h in range(3):
        keys[h] = xpose(k_ref[h])
        values[h] = xpose(v_ref[h])
        for k in range(4):
            gout[h, :, 256 * k : 256 * k + 256] = ds[k][64 * h : 64 * h + 64]
    gk[...] = jnp.zeros_like(gk)
    gv[...] = jnp.zeros_like(gv)

    def step(i, carry):
        h, b = lax.shift_right_logical(i, 2), i & 3
        at = pl.ds(pl.multiple_of(b * 256, 256), 256)
        query, grad = q_ref[h, :, at], gout[h, :, at]
        scores = dot(keys[h], query)
        column = seg_col[...]
        allowed = jnp.concatenate([column, column], axis=1) == seg_row[:, at]
        probs = jnp.where(allowed, jnp.exp(jnp.where(allowed, scores, NEGATIVE) - lse[h, :, at]), 0.0)
        gprobs = dot(values[h], grad)
        delta = jnp.sum(probs * gprobs, axis=0, keepdims=True)
        gscores = (probs * (gprobs - delta)).astype(low)
        all_rows[h, :, at] = (dot(k_ref[h], gscores) * HD**-0.5).astype(low)
        gk[h] += dot(query, gscores, NT)
        gv[h] += dot(grad, probs.astype(low), NT)
        return carry

    lax.fori_loop(0, 12, step, 0)
    all_rows[3:6] = gk[...].astype(low)
    all_rows[6:9] = gv[...].astype(low)
    all_rows[9] = jnp.zeros((64, 1024), low)


def attend_back_call(ds, queries, keys, values, lse, seg_row, seg_col):
    f32 = jnp.float32
    return pl.pallas_call(
        attend_back_kernel,
        out_shape=shape(10, 64, 1024),
        in_specs=[VM] * 10,
        out_specs=VM,
        scratch_shapes=[
            pltpu.VMEM((3, 1024, 64), jnp.bfloat16),
            pltpu.VMEM((3, 1024, 64), jnp.bfloat16),
            pltpu.VMEM((3, 64, 1024), jnp.bfloat16),
            pltpu.VMEM((3, 64, 1024), f32),
            pltpu.VMEM((3, 64, 1024), f32),
        ],
        cost_estimate=cost(12_000_000_000, 6_000_000, 3_145_728),
        name="attend_back",
    )(*ds, queries, keys, values, lse, seg_row, seg_col)


def project_back_kernel(me_ref, rows_ref, wt, xt, sums_one, sums_two, isums, *refs):
    own, b1, b2, b3, theirs, mine = refs[:6]
    canon, rel, rows, heap = refs[6:]
    low, f32, f, z = jnp.bfloat16, jnp.float32, me_ref[0], me_ref[1]
    all_rows = jnp.reshape(rows_ref[...], (640, 1024))
    for k, out in enumerate((own, b1, b2, b3)):
        part = xpose(all_rows[:, 256 * k : 256 * k + 256])
        out[...] = dot(part, wt[...]).astype(out.dtype)
    qsum = jnp.sum(all_rows[:192].astype(f32), axis=1, keepdims=True)
    vsum = jnp.sum(all_rows[384:576].astype(f32), axis=1, keepdims=True)
    rows[...] = jnp.zeros_like(rows)
    rows[66:69] = sums_one[0:3]
    rows[69:72] = sums_two[0:3]
    canon[...] = xpose(rows[...])
    for g in range(8):
        heap[g : g + 1] = isums[:, 384 * g : 384 * g + 384]
    lane = lax.broadcasted_iota(jnp.int32, (96, 128), 1)
    for c in range(4):
        part = dot(shares(c), heap[...].astype(low), NT)
        for g in range(8):
            canon[96 * g : 96 * g + 96] += jnp.where(lane == 72 + c, part[:, g : g + 1], 0.0)
    lane = lax.broadcasted_iota(jnp.int32, (192, 128), 1)
    at = pl.ds(pl.multiple_of(z * 192, 64), 192)
    canon[at] += jnp.where(lane == 64, qsum, 0.0) + jnp.where(lane == 65, vsum, 0.0)
    for kf in range(8):
        rel[96 * kf : 96 * kf + 96] = canon[pl.ds(pl.multiple_of((f ^ kf) * 96, 32), 96)]
    grads = dot(xt[...], all_rows, NT)
    heads, tail = grads[:, :512].astype(low), (grads[:, 512:] + rel[...]).astype(low)
    for kf in range(8):
        out = theirs if kf % 2 else mine
        for zz in range(4):
            rows = slice(96 * kf + 24 * zz, 96 * kf + 24 * zz + 24)
            out[kf // 2, zz, :, :512] = heads[rows]
            out[kf // 2, zz, :, 512:] = tail[rows]


def project_back_call(me, rows, wt, xt, sums_one, sums_two, isums):
    f32 = jnp.float32
    outs = [shape(256, 768, dtype=f32)] + [shape(256, 768)] * 3 + [shape(4, 4, 24, 640)] * 2
    return pl.pallas_call(
        project_back_kernel,
        out_shape=outs,
        in_specs=[SM] + [VM] * 6,
        out_specs=[VM] * len(outs),
        scratch_shapes=[
            pltpu.VMEM((768, 128), f32),
            pltpu.VMEM((768, 128), f32),
            pltpu.VMEM((128, 768), f32),
            pltpu.VMEM((8, 384), f32),
        ],
        cost_estimate=cost(5_000_000_000, 10_000_000),
        name="project_back",
    )(me, rows, wt, xt, sums_one, sums_two, isums)


def on_block(
    tokens,
    segments,
    cotangent,
    query_weight,
    query_bias,
    key_weight,
    value_weight,
    value_bias,
    mixer_weight,
    mixer_bias,
    first_gain,
    first_shift,
    inner_weight,
    inner_bias,
    outer_weight,
    outer_bias,
    second_gain,
    second_shift,
):
    f, z = lax.axis_index("fsdp"), lax.axis_index("seq")
    me = jnp.stack([f, z]).astype(jnp.int32)
    low, f32 = jnp.bfloat16, jnp.float32
    vectors = jnp.stack(
        [
            query_bias,
            value_bias,
            mixer_bias,
            first_gain,
            first_shift,
            outer_bias,
            second_gain,
            second_shift,
        ]
        + list(inner_bias.reshape(4, 24))
    )
    *messages, both, outers, seg_row, seg_col = pack_call(
        me, vectors, segments, query_weight, key_weight, value_weight, mixer_weight, inner_weight, outer_weight
    )
    got = [messages[0]] + [hop(messages[k], "seq", k, 4) for k in (1, 2, 3)]
    pieces = spread_plane(jnp.stack(got))
    outers = spread_seq(outers)
    both = spread_seq(both)
    tokens_late, *outers = after((tokens, *outers))
    xs = spread_seq(tokens_late)
    both, _ = after((jnp.stack(both), xs[1]))
    outers = spread_plane(jnp.stack(outers))
    both = spread_plane(both)

    wt, rows, ibias, bias = prepare_call(me, pieces)
    queries, keys, values, *ms, lse = attend_call(xs, wt, bias, seg_row, seg_col)
    *xs_late, ms[0] = after((*xs, ms[0]))
    xt = turn_call(me, xs_late)
    ms = [ms[0]] + [hop(ms[k], "seq", k, 4) for k in (1, 2, 3)]
    *ms, xt = after((*ms, xt))
    result, slope, first_low, normed, scale, second, gouter, sums_two, theirs, mine = feed_call(
        me, ms, tokens, cotangent, rows, ibias, both, outers
    )
    outer_mine = mine.reshape(4, 4, 96, 768)
    outer_got = hop(theirs.reshape(4, 4, 96, 768), "fsdp", 1, 8)
    residual, sums_one, isums, gin, *ds = feed_back_call(
        me, rows, slope, normed, scale, second, gouter, both, outers
    )
    ds = [ds[0]] + [hop(ds[k], "seq", k, 4) for k in (1, 2, 3)]
    gin, outer_got = after((gin, outer_got))
    outer_far = sum_far(outer_got, outer_mine)
    theirs, both_mine = feed_grad_call(me, ms, first_low, gin, residual)
    both_got = hop(theirs, "fsdp", 1, 8)
    *ds, far_y, far_x = after((*ds, *outer_far))
    outer_near = sum_near(outer_got, outer_mine, far_y, far_x)
    rows_back = attend_back_call(ds, queries, keys, values, lse, seg_row, seg_col)
    rows_back, both_got, *outer_near = after((rows_back, both_got, *outer_near))
    outer_total = outer_mine[0] + outer_got[0] + outer_near[0] + outer_near[1]
    both_far = sum_far(both_got, both_mine)
    own, one, two, three, theirs, mine = project_back_call(
        me, rows_back, wt, xt, sums_one, sums_two, isums
    )
    outer_sum = sum_place(outer_total, z)
    both_near = sum_near(both_got, both_mine, *both_far)
    both_total = both_mine[0] + both_got[0] + both_near[0] + both_near[1]
    both_sum = sum_place(both_total, z)
    grad_tokens = residual + sum_seq(two, one, three, own)
    total = sum_plane(theirs, mine)
    parts = [pick(total, z)] + [hop(pick(total, z ^ k), "seq", k, 4) for k in (1, 2, 3)]
    parts = jnp.stack(parts)
    parts = jnp.stack([pick(parts, j ^ z) for j in range(4)]).astype(f32)
    weights = [
        jnp.concatenate([parts[j, :, k * 192 : (k + 1) * 192] for j in range(4)], axis=1)
        for k in range(3)
    ]
    sums = jnp.sum(parts[:, :, 576:588], axis=0).T
    return (
        result,
        grad_tokens.astype(low),
        weights[0],
        sums[0],
        weights[1],
        weights[2],
        sums[1],
        both_sum[0],
        sums[2],
        sums[3],
        sums[4],
        both_sum[1:].swapaxes(0, 1).reshape(24, 3072),
        sums[8:].reshape(-1),
        outer_sum,
        sums[5],
        sums[6],
        sums[7],
    )


def gather_rows(own):
    return lax.all_gather(own, ("fsdp", "seq"), axis=0, tiled=True)


def reduce_all(grad):
    return lax.psum_scatter(
        grad.astype(jnp.float32), ("fsdp", "seq"), scatter_dimension=0, tiled=True
    )


def on_device(
    sizes,
    tokens,
    segments,
    cotangent,
    query_weight,
    query_bias,
    key_weight,
    value_weight,
    value_bias,
    mixer_weight,
    mixer_bias,
    first_gain,
    first_shift,
    inner_weight,
    inner_bias,
    outer_weight,
    outer_bias,
    second_gain,
    second_shift,
):
    nf, nz = sizes
    z = lax.axis_index("seq")
    low = jnp.bfloat16
    share, width = query_weight.shape
    wide = inner_weight.shape[1]
    cut = width // nz
    ratio = wide // width
    small = jnp.stack(
        [
            piece.astype(low)
            for piece in (
                query_bias,
                value_bias,
                mixer_bias,
                first_gain,
                first_shift,
                outer_bias,
                second_gain,
                second_shift,
            )
        ]
        + list(inner_bias.astype(low).reshape(ratio, share)),
        axis=1,
    )
    heads_of = [
        piece.astype(low).reshape(share, nz, cut) for piece in (query_weight, key_weight, value_weight)
    ]

    rows_all = lax.all_gather(tokens, "seq", axis=0, tiled=True)

    def message(target):
        return jnp.concatenate(
            [lax.dynamic_index_in_dim(piece, target, 1, keepdims=False) for piece in heads_of] + [small],
            axis=1,
        )

    packed = jnp.concatenate(
        [piece.astype(low) for piece in (query_weight, key_weight, value_weight)] + [small], axis=1
    )
    packed = lax.all_gather(packed, ("fsdp", "seq"), axis=0, tiled=True)
    heads_full = jnp.concatenate(
        [
            lax.dynamic_slice_in_dim(packed, k * width + z * cut, cut, axis=1)
            for k in range(3)
        ]
        + [packed[:, 3 * width :]],
        axis=1,
    )
    small_full = heads_full[:, 3 * cut :].astype(jnp.float32).T
    (qbias, vbias, mbias, gain_one, shift_one, obias, gain_two, shift_two) = [
        small_full[k] for k in range(8)
    ]
    ibias = (
        small_full[8:].reshape(ratio, nf * nz, share).swapaxes(0, 1).reshape(wide)
    )
    qbias = lax.dynamic_slice_in_dim(qbias, z * cut, cut)
    vbias = lax.dynamic_slice_in_dim(vbias, z * cut, cut)

    packed = jnp.concatenate(
        [mixer_weight.astype(low)]
        + [inner_weight[:, k * width : (k + 1) * width].astype(low) for k in range(ratio)],
        axis=0,
    )
    packed = gather_rows(packed).reshape(nf * nz, 1 + ratio, share, width)
    mixer_full = packed[:, 0].reshape(width, width)
    inner_full = jnp.concatenate(
        [packed[:, 1 + k].reshape(width, width) for k in range(ratio)], axis=1
    )
    outer_full = gather_rows(outer_weight.astype(low))

    projected = product(rows_all, heads_full[:, : 3 * cut])
    query_heads = (projected[:, :cut] + qbias).astype(low)
    key_heads = projected[:, cut : 2 * cut].astype(low)
    value_heads = (projected[:, 2 * cut :] + vbias).astype(low)
    segment = segments[0]
    mixed_heads, logsum = attend_forward(query_heads, key_heads, value_heads, segment)
    mixed_rows = lax.all_to_all(mixed_heads, "seq", split_axis=0, concat_axis=1, tiled=True)
    attended = product(mixed_rows, mixer_full) + mbias
    first_out, first_normed, first_scale = normalize(
        tokens.astype(jnp.float32) + attended, gain_one, shift_one
    )
    first_low = first_out.astype(low)
    inner_pre = product(first_low, inner_full) + ibias
    active, gelu_back = jax.vjp(lambda value: jax.nn.gelu(value, approximate=False), inner_pre)
    active_low = active.astype(low)
    outer = product(active_low, outer_full) + obias
    result, second_normed, second_scale = normalize(first_out + outer, gain_two, shift_two)
    grad_second, grad_gain_two, grad_shift_two = normalize_back(
        cotangent.astype(jnp.float32), second_normed, second_scale, gain_two
    )
    grad_outer = grad_second.astype(low)
    grad_outer_weight = product_tn(active_low, grad_outer).astype(low)
    grad_outer_bias = column_sum(grad_outer)
    outer_sum = reduce_all(grad_outer_weight)
    grad_inner = gelu_back(product_nt(grad_outer, outer_full))[0].astype(low)
    grad_inner_weight = product_tn(first_low, grad_inner).astype(low)
    grad_inner_bias = column_sum(grad_inner)
    grad_first_out = grad_second + product_nt(grad_inner, inner_full)
    grad_residual, grad_gain_one, grad_shift_one = normalize_back(
        grad_first_out, first_normed, first_scale, gain_one
    )
    grad_attended = grad_residual.astype(low)
    grad_mixer_weight = product_tn(mixed_rows, grad_attended).astype(low)
    grad_mixer_bias = column_sum(grad_attended)
    packed = jnp.concatenate(
        [grad_mixer_weight.reshape(nf * nz, 1, share, width)]
        + [
            grad_inner_weight[:, k * width : (k + 1) * width].reshape(nf * nz, 1, share, width)
            for k in range(ratio)
        ],
        axis=1,
    ).reshape(-1, width)
    packed_sum = reduce_all(packed)
    mixer_sum = packed_sum[:share]
    inner_sum = jnp.concatenate(
        [packed_sum[(1 + k) * share : (2 + k) * share] for k in range(ratio)], axis=1
    )
    grad_mixed = product_nt(grad_attended, mixer_full).astype(low)
    grad_mixed_heads = lax.all_to_all(grad_mixed, "seq", split_axis=1, concat_axis=0, tiled=True)
    grad_query_heads, grad_key_heads, grad_value_heads = attend_back(
        query_heads, key_heads, value_heads, segment, logsum, grad_mixed_heads
    )
    grads = jnp.concatenate([grad_query_heads, grad_key_heads, grad_value_heads], axis=1)
    heads_grad = product_tn(rows_all, grads).astype(low)
    zero = jnp.zeros((width,), jnp.float32)
    small_grad = jnp.stack(
        [
            lax.dynamic_update_slice_in_dim(zero, column_sum(grad_query_heads), z * cut, 0),
            lax.dynamic_update_slice_in_dim(zero, column_sum(grad_value_heads), z * cut, 0),
            grad_mixer_bias,
            grad_gain_one,
            grad_shift_one,
            grad_outer_bias,
            grad_gain_two,
            grad_shift_two,
        ]
        + list(grad_inner_bias.reshape(nf * nz, ratio, share).swapaxes(0, 1).reshape(ratio, width)),
        axis=1,
    ).astype(low)
    heads_grad = jnp.concatenate([heads_grad, small_grad], axis=1)
    mine = lax.psum_scatter(heads_grad, "fsdp", scatter_dimension=0, tiled=True)
    parts = lax.all_to_all(
        mine.reshape(nz, share, -1), "seq", split_axis=0, concat_axis=0, tiled=True
    )
    parts = parts.astype(jnp.float32)
    projections = [
        jnp.concatenate([parts[j, :, k * cut : (k + 1) * cut] for j in range(nz)], axis=1)
        for k in range(3)
    ]
    small_sum = jnp.sum(parts[:, :, 3 * cut :], axis=0).T
    back_rows = product_nt(grads, heads_full[:, : 3 * cut]).astype(low).reshape(nz, -1, width)
    back = lax.psum_scatter(back_rows, "seq", scatter_dimension=0, tiled=True)[0]
    grad_tokens = grad_residual + back
    return (
        result.astype(low),
        grad_tokens.astype(low),
        projections[0],
        small_sum[0],
        projections[1],
        projections[2],
        small_sum[1],
        mixer_sum,
        small_sum[2],
        small_sum[3],
        small_sum[4],
        inner_sum,
        small_sum[8:].reshape(-1),
        outer_sum,
        small_sum[5],
        small_sum[6],
        small_sum[7],
    )


def solution(mesh):
    placed = (
        P(("fsdp", "seq"), None),
        P("fsdp", None),
        P(("fsdp", "seq"), None),
        P(("fsdp", "seq"), None),
        P(("fsdp", "seq")),
        P(("fsdp", "seq"), None),
        P(("fsdp", "seq"), None),
        P(("fsdp", "seq")),
        P(("fsdp", "seq"), None),
        P(("fsdp", "seq")),
        P(("fsdp", "seq")),
        P(("fsdp", "seq")),
        P(("fsdp", "seq"), None),
        P(("fsdp", "seq")),
        P(("fsdp", "seq"), None),
        P(("fsdp", "seq")),
        P(("fsdp", "seq")),
        P(("fsdp", "seq")),
    )
    sizes = (mesh.shape["fsdp"], mesh.shape["seq"])
    return jax.shard_map(
        on_block if sizes == (8, 4) else functools.partial(on_device, sizes),
        mesh=mesh,
        in_specs=placed,
        out_specs=(
            P(("fsdp", "seq"), None),
            P(("fsdp", "seq"), None),
            P(("fsdp", "seq"), None),
            P(("fsdp", "seq")),
            P(("fsdp", "seq"), None),
            P(("fsdp", "seq"), None),
            P(("fsdp", "seq")),
            P(("fsdp", "seq"), None),
            P(("fsdp", "seq")),
            P(("fsdp", "seq")),
            P(("fsdp", "seq")),
            P(("fsdp", "seq"), None),
            P(("fsdp", "seq")),
            P(("fsdp", "seq"), None),
            P(("fsdp", "seq")),
            P(("fsdp", "seq")),
            P(("fsdp", "seq")),
        ),
        check_vma=False,
    )
```
